32 devices in a mesh: dp: 2 (over x), sp: 16 (over y, z, core).
Axes of the slice: x: 2, y: 2, z: 4, core: 2. Of those that a mesh axis runs over, the one named last changes fastest.
Arguments:
- x: bfloat16 [4096, 14336], P(('dp', 'sp')), parts along dimension 0
- gain: bfloat16 [14336], replicated
- wq: bfloat16 [14336, 14336], replicated
- wk: bfloat16 [14336, 14336], replicated
- wv: bfloat16 [14336, 14336], replicated
- wo: bfloat16 [14336, 14336], replicated
Outputs:
- output: bfloat16 [4096, 14336], P(('dp', 'sp')), parts along dimension 0
There are 2 independent parts. The reference program is written for one: setup_inputs(seed, part) draws one part's arguments, and reference() takes and returns one part's arrays. A program takes and returns all parts, laid end to end along the dimension named above; an argument that names none is the same for every part.
All inputs are finite; a program needn't handle non-finite values.
Results may differ from the reference program's by a relative error of at most 0.012.
Values are sent between devices in bfloat16 or wider.
A program may use at most 3.75 GiB of HBM per device.

```python
import jax
import jax.numpy as jnp
from jax import lax

ROWS = 2048
D = 14336
HEADS = 112
KV_HEADS = 112
HEAD = 128
THETA = 10000


def setup_inputs(seed: int = 0, part: int = 0) -> dict:
    kx, kn, kq, kk, kv, ko = jax.random.split(jax.random.key(seed), 6)

    def weights(key, rows, columns):
        return jax.random.normal(key, (rows, columns), jnp.float32) * rows**-0.5

    drawn = {
        "x": jax.random.normal(jax.random.fold_in(kx, part), (ROWS, D), jnp.float32),
        "gain": 1 + 0.1 * jax.random.normal(kn, (D,), jnp.float32),
        "wq": 2 * weights(kq, D, HEADS * HEAD),
        "wk": 2 * weights(kk, D, KV_HEADS * HEAD),
        "wv": 4 * weights(kv, D, KV_HEADS * HEAD),
        "wo": weights(ko, HEADS * HEAD, D),
    }
    return {k: v.astype(jnp.bfloat16) for k, v in drawn.items()}


def normed(x, gain):
    wide = x.astype(jnp.float32)
    scale = lax.rsqrt(jnp.mean(wide * wide, -1, keepdims=True) + 1e-6)
    return (wide * scale * gain.astype(jnp.float32)).astype(jnp.bfloat16)


def turned(t, place, theta):
    half = t.shape[-1] // 2
    angle = place.astype(jnp.float32)[:, None] * theta ** (-jnp.arange(half, dtype=jnp.float32) / half)
    cos, sin = jnp.cos(angle)[:, None], jnp.sin(angle)[:, None]
    a, b = t[..., :half].astype(jnp.float32), t[..., half:].astype(jnp.float32)
    return jnp.concatenate([a * cos - b * sin, b * cos + a * sin], -1).astype(jnp.bfloat16)


def matmul(a, w):
    return jnp.dot(a, w, preferred_element_type=jnp.float32).astype(jnp.bfloat16)


def einsum(form, a, b):
    return jnp.einsum(form, a.astype(jnp.float32), b.astype(jnp.float32))


def attention(q, k, v):
    scores = einsum("tgsd,ugd->gstu", q, k) * q.shape[-1] ** -0.5
    token = jnp.arange(q.shape[0])
    scores = jnp.where(token[:, None] >= token, scores, -jnp.inf)
    weights = jax.nn.softmax(scores, -1).astype(jnp.bfloat16)
    return einsum("gstu,ugd->tgsd", weights, v).astype(jnp.bfloat16)


def reference(x, gain, wq, wk, wv, wo):
    a, place = normed(x, gain), jnp.arange(ROWS)
    q = turned(matmul(a, wq).reshape(ROWS, HEADS, HEAD), place, THETA).reshape(ROWS, KV_HEADS, -1, HEAD)
    k = turned(matmul(a, wk).reshape(ROWS, KV_HEADS, HEAD), place, THETA)
    v = matmul(a, wv).reshape(ROWS, KV_HEADS, HEAD)
    seen = attention(q, k, v).reshape(ROWS, HEADS * HEAD)
    return (x.astype(jnp.float32) + jnp.dot(seen, wo, preferred_element_type=jnp.float32)).astype(jnp.bfloat16)
```

```python
import functools

import jax
import jax.numpy as jnp
from jax import lax
from jax.experimental import pallas as pl
from jax.experimental.pallas import tpu as pltpu
from jax.sharding import PartitionSpec as P

HEAD = 128
THETA = 10000
LOG2E = 1.4426950408889634
D = 14336
OWN = 128
PAIR = 2 * OWN
CHIPS = 8
SEQ = PAIR * CHIPS
HALF = D // 2
HEADS = 7
WIDE = HEADS * HEAD
VMEM = 63 * 2**20
BF, F32 = jnp.bfloat16, jnp.float32


def normed(x, gain):
    wide = x.astype(F32)
    scale = lax.rsqrt(jnp.mean(wide * wide, -1, keepdims=True) + 1e-6)
    return (wide * scale * gain.astype(F32)).astype(BF)


def partner(chip, t):
    y, h, z = chip // 4, (chip // 2) % 2, chip % 2
    y = (y + 1 - t % 2) % 2
    z = (z + 1 - (t // 2) % 2) % 2
    h = (h + 1 - t // 4) % 2
    return y * 4 + h * 2 + z


def turn_of(chip, t):
    end = 1 - (chip // 2 + chip) % 2
    return t // 7 * 7 + (1 - t // 7) * ((t + 4 * end) % 7)


def greet_chips(chip, core):
    barrier = pltpu.get_barrier_semaphore()
    for t in range(CHIPS - 1):
        pl.semaphore_signal(barrier, inc=1, device_id={"sp": partner(chip, t) * 2 + core})
    return barrier


PARTS = 4
DEEP = D // PARTS
SLOTS = 3
TILES = 3 * CHIPS


def _qkv(a_ref, cos_ref, sin_ref, wq, wk, wv, out_ref, a_v, w_v, acc, stage, a_sem, a_send, a_recv, w_sem, send, recv, keep):
    me = lax.axis_index("sp")
    core, chip = me % 2, me // 2
    other = chip * 2 + 1 - core
    steps = TILES * PARTS

    def weights(i, start):
        tile, part, slot = i // PARTS, i % PARTS, i % SLOTS
        t, j = turn_of(chip, tile // 3), tile % 3
        col = pl.multiple_of(core * HALF + partner(chip, t) * WIDE, HEAD)
        row = pl.multiple_of(part * DEEP, DEEP)
        for n, w in enumerate((wq, wk, wv)):

            @pl.when(j == n)
            def _():
                copy = pltpu.make_async_copy(w.at[pl.ds(row, DEEP), pl.ds(col, WIDE)], w_v.at[slot], w_sem.at[slot])
                if start:
                    copy.start()
                else:
                    copy.wait()

    for i in range(SLOTS - 1):
        weights(i, True)
    barrier = greet_chips(chip, core)
    pl.semaphore_signal(barrier, inc=1, device_id={"sp": other})
    pl.semaphore_wait(barrier, CHIPS)

    mine = pl.ds(pl.multiple_of(core * OWN, OWN), OWN)

    def rows(part, remote):
        cols = pl.ds(pl.multiple_of(part * DEEP, DEEP), DEEP)
        src, dst = a_ref.at[:, cols], a_v.at[mine, cols]
        if remote:
            return pltpu.make_async_remote_copy(src, dst, a_send.at[part], a_recv.at[part], device_id={"sp": other})
        return pltpu.make_async_copy(src, dst, a_sem.at[part])

    for part in range(PARTS):
        rows(part, True).start()
        rows(part, False).start()
    acc[...] = jnp.zeros_like(acc)

    def away(tile):
        t, j = turn_of(chip, tile // 3), tile % 3
        dst = out_ref.at[j, :, pl.ds(pl.multiple_of(chip * PAIR, PAIR), PAIR), :]
        return pltpu.make_async_remote_copy(
            stage.at[tile], dst, send.at[t, j], recv.at[t, j], device_id={"sp": partner(chip, t) * 2 + core}
        )

    def here(tile):
        dst = out_ref.at[tile % 3, :, pl.ds(pl.multiple_of(chip * PAIR, PAIR), PAIR), :]
        return pltpu.make_async_copy(stage.at[tile], dst, keep.at[tile % 3])

    def body(i, _):
        tile, part = i // PARTS, i % PARTS

        @pl.when(i + SLOTS - 1 < steps)
        def _():
            weights(i + SLOTS - 1, True)

        @pl.when(i < PARTS)
        def _():
            rows(part, True).wait()
            rows(part, False).wait()

        weights(i, False)
        cols = pl.ds(pl.multiple_of(part * DEEP, DEEP), DEEP)
        acc[...] += jnp.dot(a_v[:, cols], w_v[i % SLOTS], preferred_element_type=F32)

        @pl.when(part == PARTS - 1)
        def _():
            turn = tile % 3 < 2

            @pl.when(turn)
            def _():
                cos, sin = cos_ref[...], sin_ref[...]
                for n in range(HEADS):
                    v = acc[:, n * HEAD : (n + 1) * HEAD].astype(BF).astype(F32)
                    stage[tile, n] = (v * cos + pltpu.roll(v, HEAD // 2, 1) * sin).astype(BF)

            @pl.when(jnp.logical_not(turn))
            def _():
                for n in range(HEADS):
                    stage[tile, n] = acc[:, n * HEAD : (n + 1) * HEAD].astype(BF)

            acc[...] = jnp.zeros_like(acc)

            @pl.when(tile < TILES - 3)
            def _():
                away(tile).start()

            @pl.when(tile >= TILES - 3)
            def _():
                here(tile).start()

        return 0

    lax.fori_loop(0, steps, body, 0)

    def finish(tile, _):
        away(tile).wait()
        return 0

    lax.fori_loop(0, TILES - 3, finish, 0)
    for tile in range(TILES - 3, TILES):
        here(tile).wait()


def qkv(a, cos, sin, wq, wk, wv):
    hbm, vmem = pl.BlockSpec(memory_space=pl.ANY), pl.BlockSpec(memory_space=pltpu.VMEM)
    dma = pltpu.SemaphoreType.DMA
    return pl.pallas_call(
        _qkv,
        out_shape=jax.ShapeDtypeStruct((3, HEADS, SEQ, HEAD), BF),
        in_specs=[hbm, vmem, vmem, hbm, hbm, hbm],
        out_specs=hbm,
        scratch_shapes=[
            pltpu.VMEM((PAIR, D), BF),
            pltpu.VMEM((SLOTS, DEEP, WIDE), BF),
            pltpu.VMEM((PAIR, WIDE), F32),
            pltpu.VMEM((TILES, HEADS, PAIR, HEAD), BF),
            dma((PARTS,)),
            dma((PARTS,)),
            dma((PARTS,)),
            dma((SLOTS,)),
            dma((CHIPS - 1, 3)),
            dma((CHIPS - 1, 3)),
            dma((3,)),
        ],
        compiler_params=pltpu.CompilerParams(collective_id=0, has_side_effects=True, vmem_limit_bytes=VMEM),
        name="qkv",
    )(a, cos, sin, wq, wk, wv)


LAG = 2
SPAN = 1792
COLS = D // SPAN
W_SLOTS = 3


def _finish(states, x_ref, wo, y_ref, heads_v, stage, o_v, w_v, sums, theirs, h_sem, w_sem, send, recv, p_send, p_recv):
    me = lax.axis_index("sp")
    core, chip = me % 2, me // 2
    other = chip * 2 + 1 - core
    e = HEAD**-0.5 * LOG2E

    def head(n):
        return pltpu.make_async_copy(states.at[:, n], heads_v.at[n % 2], h_sem.at[n % 2])

    def weights(m):
        cols = pl.ds(pl.multiple_of(m % COLS * SPAN, SPAN), SPAN)
        slot = m % W_SLOTS
        return pltpu.make_async_copy(wo.at[pl.ds(core * CHIPS, CHIPS), m // COLS, :, cols], w_v.at[slot], w_sem.at[slot])

    head(0).start()
    for m in range(W_SLOTS - 1):
        weights(m).start()
    barrier = greet_chips(chip, core)
    pl.semaphore_signal(barrier, inc=1, device_id={"sp": other})
    pl.semaphore_wait(barrier, CHIPS)

    block = pl.ds(pl.multiple_of(chip * HEAD, HEAD), HEAD)

    def away(n, t):
        to = partner(chip, t)
        return pltpu.make_async_remote_copy(
            stage.at[n, to], o_v.at[n, :, block], send.at[n, t], recv.at[n, t], device_id={"sp": to * 2 + core}
        )

    def swap(i):
        src = sums.at[i, pl.ds(pl.multiple_of((1 - core) * OWN, OWN), OWN), :]
        return pltpu.make_async_remote_copy(src, theirs.at[i], p_send.at[i], p_recv.at[i], device_id={"sp": other})

    def close(i):
        swap(i).wait()
        mine = sums[i, pl.ds(pl.multiple_of(core * OWN, OWN), OWN), :]
        cols = pl.ds(pl.multiple_of(i * SPAN, SPAN), SPAN)
        y_ref[:, cols] = (x_ref[:, cols].astype(F32) + (mine + theirs[i])).astype(BF)

    def zero(i, _):
        sums[i] = jnp.zeros((PAIR, SPAN), F32)
        return 0

    lax.fori_loop(0, COLS, zero, 0)
    low = lax.broadcasted_iota(jnp.int32, (PAIR, PAIR), 0) >= lax.broadcasted_iota(jnp.int32, (PAIR, PAIR), 1)

    def attention(n):
        @pl.when(n + 1 < HEADS)
        def _():
            head(n + 1).start()

        head(n).wait()
        at = n % 2
        for i in range(CHIPS):
            here = slice(i * PAIR, (i + 1) * PAIR)
            q = heads_v[at, 0, here, :]
            near = lax.dot_general(q, heads_v[at, 1, here, :], (((1,), (1,)), ((), ())), preferred_element_type=F32)
            near = jnp.where(low, near, -jnp.inf)
            top = near.max(axis=1, keepdims=True)
            if i:
                far = lax.dot_general(q, heads_v[at, 1, : i * PAIR, :], (((1,), (1,)), ((), ())), preferred_element_type=F32)
                top = jnp.maximum(top, far.max(axis=1, keepdims=True))
            p = jnp.exp2((near - top) * e)
            total = p.sum(axis=1, keepdims=True)
            o = jnp.dot(p.astype(BF), heads_v[at, 2, here, :], preferred_element_type=F32)
            if i:
                p = jnp.exp2((far - top) * e)
                total += p.sum(axis=1, keepdims=True)
                o += jnp.dot(p.astype(BF), heads_v[at, 2, : i * PAIR, :], preferred_element_type=F32)
            stage[n, i] = (o * (1 / total)).astype(BF)
        for t in range(CHIPS - 1):
            away(n, turn_of(chip, t)).start()
        o_v[n, :, block] = stage[n, chip]

    def projection(j):
        for t in range(CHIPS - 1):
            away(j, t).wait()

        def tile(i, _):
            m = j * COLS + i

            @pl.when(m + W_SLOTS - 1 < HEADS * COLS)
            def _():
                weights(m + W_SLOTS - 1).start()

            weights(m).wait()
            w = w_v[m % W_SLOTS].reshape(CHIPS * HEAD, SPAN)
            sums[i] += jnp.dot(o_v[j], w, preferred_element_type=F32)

            @pl.when(j == HEADS - 1)
            def _():
                swap(i).start()

            @pl.when((j == HEADS - 1) & (i > 0))
            def _():
                close(i - 1)

            return 0

        lax.fori_loop(0, COLS, tile, 0)

    def body(s, _):
        @pl.when(s < HEADS)
        def _():
            attention(s)

        @pl.when(s >= LAG)
        def _():
            projection(s - LAG)

        return 0

    lax.fori_loop(0, HEADS + LAG, body, 0)
    close(COLS - 1)


def finish(states, x, wo):
    hbm, vmem = pl.BlockSpec(memory_space=pl.ANY), pl.BlockSpec(memory_space=pltpu.VMEM)
    dma = pltpu.SemaphoreType.DMA
    return pl.pallas_call(
        _finish,
        out_shape=jax.ShapeDtypeStruct((OWN, D), BF),
        in_specs=[hbm, vmem, hbm],
        out_specs=vmem,
        scratch_shapes=[
            pltpu.VMEM((2, 3, SEQ, HEAD), BF),
            pltpu.VMEM((HEADS, CHIPS, PAIR, HEAD), BF),
            pltpu.VMEM((HEADS, PAIR, CHIPS * HEAD), BF),
            pltpu.VMEM((W_SLOTS, CHIPS, HEAD, SPAN), BF),
            pltpu.VMEM((COLS, PAIR, SPAN), F32),
            pltpu.VMEM((COLS, OWN, SPAN), F32),
            dma((2,)),
            dma((W_SLOTS,)),
            dma((HEADS, CHIPS - 1)),
            dma((HEADS, CHIPS - 1)),
            dma((COLS,)),
            dma((COLS,)),
        ],
        compiler_params=pltpu.CompilerParams(collective_id=1, has_side_effects=True, vmem_limit_bytes=VMEM),
        name="finish",
    )(states, x, wo.reshape(2 * CHIPS, HEADS, HEAD, D))


def solution(mesh):
    def step(x, gain, wq, wk, wv, wo):
        first = lax.axis_index("sp") // 2 * PAIR
        half = HEAD // 2
        angle = (first + jnp.arange(PAIR)).astype(F32)[:, None] * THETA ** (-jnp.arange(half, dtype=F32) / half)
        cos, sin = jnp.cos(angle), jnp.sin(angle)
        cos, sin = jnp.concatenate([cos, cos], -1), jnp.concatenate([-sin, sin], -1)
        states = qkv(normed(x, gain), cos, sin, wq, wk, wv)
        return finish(states, x, wo)

    tokens, whole = P(("dp", "sp"), None), P(None, None)
    return jax.shard_map(
        step,
        mesh=mesh,
        in_specs=(tokens, P(None), whole, whole, whole, whole),
        out_specs=tokens,
        check_vma=False,
    )
```
